32 devices in a mesh: rep: 2 (over z, core), dp: 16 (over x, y).
Axes of the slice: x: 4, y: 4, z: 1, core: 2. Of those that a mesh axis runs over, the one named last changes fastest.
The devices are a block of a 4x4x8 slice.
Arguments:
- a: bfloat16 [32, 4, 4096, 512], P(('rep', 'dp')), parts along dimension 0
- g: bfloat16 [32, 4, 4096, 1664], P(('rep', 'dp')), parts along dimension 0
Outputs:
- output: bfloat16 [8, 512, 1664], P('rep'), parts along dimension 0
There are 2 independent parts. The reference program is written for one: setup_inputs(seed, part) draws one part's arguments, and reference() takes and returns one part's arrays. A program takes and returns all parts, laid end to end along the dimension named above; each array names one.
All inputs are finite; a program needn't handle non-finite values.
Results may differ from the reference program's by a relative error of at most 0.012.
Values are sent between devices in bfloat16 or wider.
A program may use at most 768 MiB of HBM per device.

```python
import jax
import jax.numpy as jnp
from jax import lax

DEVICES = 16
MATRICES = 4
TOKENS = 4096
D = 512
FF = 1664


def setup_inputs(seed: int = 0, part: int = 0) -> dict:
    ka, kg, ks = (jax.random.fold_in(k, part) for k in jax.random.split(jax.random.key(seed), 3))
    size = 2.0 ** jax.random.uniform(ks, (DEVICES, MATRICES, 1, 1), jnp.float32, -1.0, 1.0)
    a = jax.random.normal(ka, (DEVICES, MATRICES, TOKENS, D), jnp.float32)
    g = size * jax.random.normal(kg, (DEVICES, MATRICES, TOKENS, FF), jnp.float32) * (DEVICES * TOKENS) ** -0.5
    return {"a": a.astype(jnp.bfloat16), "g": g.astype(jnp.bfloat16)}


def reference(a, g):
    def take(so_far, one):
        return so_far + jnp.einsum("ntd,ntf->ndf", *one, preferred_element_type=jnp.float32), None

    return lax.scan(take, jnp.zeros((MATRICES, D, FF), jnp.float32), (a, g))[0].astype(jnp.bfloat16)
```

```python
import functools

import jax
import jax.numpy as jnp
from jax import lax
from jax.experimental import pallas as pl
from jax.experimental.pallas import tpu as pltpu
from jax.sharding import PartitionSpec as P

MESH = pl.DeviceIdType.MESH
SIDE = 4
LANES = 128
TILES = (4, 4, 5)
LAG = (0, 2, 4, 6, 8, 10, 12, 14, 16)
K_PARTS = 2


def kernel(a_hbm, g_hbm, o_hbm, a_buf, g_buf, terms, s0, r1, s1, r2, rows, s2, r3, s3, r4, out,
           a_sem, g_sem, send_sem, recv_sem, out_sem):
    count, tokens, d_model = a_hbm.shape
    columns = []
    for t in TILES:
        columns.append((sum(w for _, w in columns), t * LANES))
    per = len(columns)
    half_rows = d_model // 2
    block = half_rows // SIDE
    side_rows = block // 2
    sub = block // SIDE
    part = tokens // K_PARTS

    me = lax.axis_index("dp")
    px, py = me // SIDE, me % SIDE

    def wrap(p):
        return (p + 2 * SIDE) % SIDE

    first = (px, py)
    second = (py, px)

    def at_first(h, p):
        return {"dp": wrap(p) * SIDE + py if h == 0 else px * SIDE + wrap(p)}

    def at_second(h, p):
        return {"dp": px * SIDE + wrap(p) if h == 0 else wrap(p) * SIDE + py}

    def of(h, p, q=0):
        return pl.multiple_of(h * half_rows + wrap(p) * block + wrap(q) * sub, sub)

    def a_load(n, k):
        slot = n % 2
        return pltpu.make_async_copy(
            a_hbm.at[n, pl.ds(k * part, part)], a_buf.at[slot, pl.ds(k * part, part)], a_sem.at[slot, k])

    def g_load(n, j, k):
        c, w = columns[j]
        slot = (n * per + j) % 2
        return pltpu.make_async_copy(
            g_hbm.at[n, pl.ds(k * part, part), pl.ds(c, w)],
            g_buf.at[slot, pl.ds(k * part, part), pl.ds(0, w)], g_sem.at[slot, k])

    for k in range(K_PARTS):
        a_load(0, k).start()
        g_load(0, 0, k).start()

    barrier = pltpu.get_barrier_semaphore()
    for d in (1, -1):
        pl.semaphore_signal(barrier, inc=1, device_id=at_first(0, px + d), device_id_type=MESH)
        pl.semaphore_signal(barrier, inc=1, device_id=at_second(0, py + d), device_id_type=MESH)

    pl.semaphore_wait(barrier, SIDE)

    def matmul(n, j):
        c, w = columns[j]
        slot, a_slot = (n * per + j) % 2, n % 2
        if j == 0:
            @pl.when(n + 1 < count)
            def _():
                for k in range(K_PARTS):
                    a_load(n + 1, k).start()
        if j + 1 < per:
            for k in range(K_PARTS):
                g_load(n, j + 1, k).start()
        else:
            @pl.when(n + 1 < count)
            def _():
                for k in range(K_PARTS):
                    g_load(n + 1, 0, k).start()

        for k in range(K_PARTS):
            if j == 0:
                a_load(n, k).wait()
            g_load(n, j, k).wait()

        def over(k, _):
            k0 = pl.multiple_of(k * part, part)
            term = lax.dot_general(
                a_buf[a_slot, pl.ds(k0, part), :], g_buf[slot, pl.ds(k0, part), pl.ds(0, w)],
                (((0,), (0,)), ((), ())), preferred_element_type=jnp.float32)

            @pl.when(k == 0)
            def _():
                terms[n, :, pl.ds(c, w)] = term

            @pl.when(k > 0)
            def _():
                terms[n, :, pl.ds(c, w)] += term
            return 0

        lax.fori_loop(0, K_PARTS, over, 0)

    def stages(n, j):
        c, w = columns[j]
        cols = pl.ds(c, w)
        unit = n * per + j

        def term(row, size):
            return terms[n, pl.ds(row, size), cols]

        def send(h, src, dst, kind, device):
            pltpu.make_async_remote_copy(
                src_ref=src, dst_ref=dst, send_sem=send_sem.at[2 * unit + h], recv_sem=recv_sem.at[kind, 2 * unit + h],
                device_id=device, device_id_type=MESH).start()

        def arrived(h, kind, size):
            ref = out.at[n, pl.ds(0, size), cols]
            pltpu.make_async_copy(ref, ref, recv_sem.at[kind, 2 * unit + h]).wait()

        def at(buf, h, i, size):
            return buf.at[n, h, pl.ds(i * size, size), cols]

        def place(row, size):
            return out.at[n, pl.ds(row, size), cols]

        def turn(h):
            return 1 - 2 * ((unit + h) % 2)

        half = side_rows

        def stage0():
            for h in (0, 1):
                p = first[h]
                s0[n, h, pl.ds(0, block), cols] = term(of(h, p + 2), block).astype(jnp.bfloat16)
                s0[n, h, pl.ds(2 * half, half), cols] = term(of(h, p - 1) + half, half).astype(jnp.bfloat16)
                s0[n, h, pl.ds(3 * half, half), cols] = term(of(h, p + 1), half).astype(jnp.bfloat16)
                send(h, at(s0, h, 0, half), at(r1, h, 0, half), 0, at_first(h, p - 1))
                send(h, at(s0, h, 1, half), at(r1, h, 1, half), 0, at_first(h, p + 1))
                send(h, at(s0, h, 2, half), at(r2, h, 3, half), 1, at_first(h, p - 1))
                send(h, at(s0, h, 3, half), at(r2, h, 2, half), 1, at_first(h, p + 1))

        def stage1():
            for h in (0, 1):
                p = first[h]
                arrived(h, 0, 2 * half)
                got = r1[n, h, :, cols].astype(jnp.float32)
                s1[n, h, pl.ds(0, half), cols] = (got[:half] + term(of(h, p - 1), half)).astype(jnp.bfloat16)
                s1[n, h, pl.ds(half, half), cols] = (got[half:] + term(of(h, p + 1) + half, half)).astype(jnp.bfloat16)
                send(h, at(s1, h, 0, half), at(r2, h, 0, half), 1, at_first(h, p - 1))
                send(h, at(s1, h, 1, half), at(r2, h, 1, half), 1, at_first(h, p + 1))

        def stage2():
            for h in (0, 1):
                p, q, t = first[h], second[h], turn(h)
                arrived(h, 1, 4 * half)
                got = r2[n, h, :, cols].astype(jnp.float32)
                rows[n, h, :, cols] = got[:block] + got[block:] + term(of(h, p), block)

                def mine(i):
                    return rows[n, h, pl.ds(pl.multiple_of(wrap(i) * sub, sub), sub), cols].astype(jnp.bfloat16)

                s2[n, h, pl.ds(0, sub), cols] = mine(q + 2)
                s2[n, h, pl.ds(sub, sub), cols] = mine(q + t)
                send(h, at(s2, h, 0, sub), at(r3, h, 0, sub), 2, at_second(h, q - t))
                send(h, at(s2, h, 1, sub), at(r4, h, 1, sub), 3, at_second(h, q + t))

        def stage3():
            for h in (0, 1):
                q, t = second[h], turn(h)
                arrived(h, 2, sub)
                got = r3[n, h, :, cols].astype(jnp.float32)
                s3[n, h, :, cols] = (
                    got + rows[n, h, pl.ds(pl.multiple_of(wrap(q - t) * sub, sub), sub), cols]).astype(jnp.bfloat16)
                send(h, at(s3, h, 0, sub), at(r4, h, 0, sub), 3, at_second(h, q - t))

        def stage4():
            for h in (0, 1):
                p, q = first[h], second[h]
                arrived(h, 3, 2 * sub)
                got = r4[n, h, :, cols].astype(jnp.float32)
                total = got[:sub] + got[sub:] + rows[n, h, pl.ds(pl.multiple_of(q * sub, sub), sub), cols]
                row = of(h, p, q)
                out[n, pl.ds(row, sub), cols] = total.astype(jnp.bfloat16)
                for d in (1, -1):
                    send(h, place(row, sub), place(row, sub), 4, at_second(h, q + d))

        def stage5():
            for h in (0, 1):
                p, q, t = first[h], second[h], turn(h)
                arrived(h, 4, 2 * sub)
                row = of(h, p, q - t)
                send(h, place(row, sub), place(row, sub), 5, at_second(h, q + t))

        def stage6():
            for h in (0, 1):
                p = first[h]
                arrived(h, 5, sub)
                row = of(h, p)
                for d in (1, -1):
                    send(h, place(row, block), place(row, block), 6, at_first(h, p + d))

        def stage7():
            for h in (0, 1):
                p = first[h]
                arrived(h, 6, 2 * block)
                row = of(h, p - 1)
                send(h, place(row, half), place(row, half), 7, at_first(h, p + 1))
                row = of(h, p + 1) + half
                send(h, place(row, half), place(row, half), 7, at_first(h, p - 1))

        def stage8():
            for h in (0, 1):
                arrived(h, 7, 2 * half)
            pltpu.make_async_copy(out.at[n, :, cols], o_hbm.at[n, :, cols], out_sem.at[unit]).start()

        return stage0, stage1, stage2, stage3, stage4, stage5, stage6, stage7, stage8

    def step(it, _):
        for j in range(per):
            for s in range(len(LAG) - 1, 0, -1):
                back = (LAG[s] - j + per - 1) // per
                jj = (j - LAG[s]) % per
                n = it - back

                @pl.when((n >= 0) & (n < count))
                def _():
                    stages(n, jj)[s]()

            @pl.when(it < count)
            def _():
                matmul(it, j)
                stages(it, j)[0]()
        return 0

    lax.fori_loop(0, count + -(-LAG[-1] // per), step, 0)

    sent = 15 * half_rows // 8
    def finish(n, _):
        for j, (c, w) in enumerate(columns):
            unit = n * per + j
            for h in (0, 1):
                ref = out.at[n, pl.ds(0, sent), pl.ds(c, w)]
                pltpu.make_async_copy(ref, ref, send_sem.at[2 * unit + h]).wait()
            pltpu.make_async_copy(out.at[n, :, pl.ds(c, w)], o_hbm.at[n, :, pl.ds(c, w)], out_sem.at[unit]).wait()
        return 0

    lax.fori_loop(0, count, finish, 0)


def solution(mesh):
    def step(a, g):
        a, g = a.reshape(a.shape[1:]), g.reshape(g.shape[1:])
        count, tokens, d_model = a.shape
        ff = g.shape[2]
        assert mesh.shape["dp"] == SIDE * SIDE and sum(TILES) * LANES == ff
        units = count * len(TILES)
        bf16, f32 = jnp.bfloat16, jnp.float32
        half_rows = d_model // 2
        block = half_rows // SIDE
        sub = block // SIDE
        VMEM, DMA = pltpu.VMEM, pltpu.SemaphoreType.DMA
        return pl.pallas_call(
            kernel,
            out_shape=jax.ShapeDtypeStruct((count, d_model, ff), bf16),
            in_specs=[pl.BlockSpec(memory_space=pl.ANY)] * 2,
            out_specs=pl.BlockSpec(memory_space=pl.ANY),
            scratch_shapes=[
                VMEM((2, tokens, d_model), bf16),
                VMEM((2, tokens, max(TILES) * LANES), bf16),
                VMEM((count, d_model, ff), f32),
                VMEM((count, 2, 2 * block, ff), bf16),
                VMEM((count, 2, block, ff), bf16),
                VMEM((count, 2, block, ff), bf16),
                VMEM((count, 2, 2 * block, ff), bf16),
                VMEM((count, 2, block, ff), f32),
                VMEM((count, 2, 2 * sub, ff), bf16),
                VMEM((count, 2, sub, ff), bf16),
                VMEM((count, 2, sub, ff), bf16),
                VMEM((count, 2, 2 * sub, ff), bf16),
                VMEM((count, d_model, ff), bf16),
                DMA((2, K_PARTS)),
                DMA((2, K_PARTS)),
                DMA((2 * units,)),
                DMA((8, 2 * units)),
                DMA((units,)),
            ],
            compiler_params=pltpu.CompilerParams(
                collective_id=0, has_side_effects=True, vmem_limit_bytes=67043328),
            name="sums",
        )(a, g)

    return jax.shard_map(
        step, mesh=mesh, in_specs=(P(("rep", "dp")), P(("rep", "dp"))), out_specs=P("rep"), check_vma=False)
```

```python
import functools

import jax
import jax.numpy as jnp
from jax import lax
from jax.experimental import pallas as pl
from jax.experimental.pallas import tpu as pltpu
from jax.sharding import PartitionSpec as P

MESH = pl.DeviceIdType.MESH
SIDE = 4
LANES = 128
TILES = (7, 6)
LAG = (0, 3, 6, 9, 12, 15, 18, 21, 24)


def kernel(a_hbm, g_hbm, out, a_buf, g_buf, terms, s0, r1, s1, r2, rows, s2, r3, s3, r4,
           a_sem, g_sem, send_sem, recv_sem):
    count, tokens, d_model = a_hbm.shape
    columns = []
    for t in TILES:
        columns.append((sum(w for _, w in columns), t * LANES))
    per = len(columns)
    half_rows = d_model // 2
    block = half_rows // SIDE
    side_rows = block // 2
    sub = block // SIDE

    me = lax.axis_index("dp")
    px, py = me // SIDE, me % SIDE

    def wrap(p):
        return (p + 2 * SIDE) % SIDE

    first = (px, py)
    second = (py, px)

    def at_first(h, p):
        return {"dp": wrap(p) * SIDE + py if h == 0 else px * SIDE + wrap(p)}

    def at_second(h, p):
        return {"dp": px * SIDE + wrap(p) if h == 0 else wrap(p) * SIDE + py}

    def of(h, p, q=0):
        return pl.multiple_of(h * half_rows + wrap(p) * block + wrap(q) * sub, sub)

    def a_load(n, h):
        rows_of = pl.ds(h * half_rows, half_rows)
        return pltpu.make_async_copy(a_hbm.at[n, :, rows_of], a_buf.at[n % 2, :, rows_of], a_sem.at[n % 2, h])

    def g_load(n, j):
        c, w = columns[j]
        slot = (n * per + j) % 2
        return pltpu.make_async_copy(g_hbm.at[n, :, pl.ds(c, w)], g_buf.at[slot, :, pl.ds(0, w)], g_sem.at[slot])

    a_load(0, 0).start()
    g_load(0, 0).start()
    a_load(0, 1).start()

    barrier = pltpu.get_barrier_semaphore()
    for d in (1, -1):
        pl.semaphore_signal(barrier, inc=1, device_id=at_first(0, px + d), device_id_type=MESH)
        pl.semaphore_signal(barrier, inc=1, device_id=at_second(0, py + d), device_id_type=MESH)

    pl.semaphore_wait(barrier, SIDE)

    def matmul(n, j, h):
        c, w = columns[j]
        if j == 0:
            a_load(n, h).wait()

            @pl.when(n + 1 < count)
            def _():
                a_load(n + 1, h).start()
        if h == 0:
            g_load(n, j).wait()
            if j + 1 < per:
                g_load(n, j + 1).start()
            else:
                @pl.when(n + 1 < count)
                def _():
                    g_load(n + 1, 0).start()
        mine = pl.ds(h * half_rows, half_rows)
        terms[n, mine, pl.ds(c, w)] = lax.dot_general(
            a_buf[n % 2, :, mine], g_buf[(n * per + j) % 2, :, pl.ds(0, w)],
            (((0,), (0,)), ((), ())), preferred_element_type=jnp.float32)

    def stages(n, j, h):
        c, w = columns[j]
        cols = pl.ds(c, w)
        unit = n * per + j

        def term(row, size):
            return terms[n, pl.ds(row, size), cols]

        def send(h, src, dst, kind, device):
            pltpu.make_async_remote_copy(
                src_ref=src, dst_ref=dst, send_sem=send_sem.at[2 * unit + h], recv_sem=recv_sem.at[kind, 2 * unit + h],
                device_id=device, device_id_type=MESH).start()

        def arrived(h, kind, size):
            ref = out.at[n, pl.ds(0, size), cols]
            pltpu.make_async_copy(ref, ref, recv_sem.at[kind, 2 * unit + h]).wait()

        def at(buf, h, i, size):
            return buf.at[n, h, pl.ds(i * size, size), cols]

        def place(row, size):
            return out.at[n, pl.ds(row, size), cols]

        def turn(h):
            return 1 - 2 * ((unit + h) % 2)

        half = side_rows

        def stage0():
            p = first[h]
            s0[n, h, pl.ds(0, block), cols] = term(of(h, p + 2), block).astype(jnp.bfloat16)
            s0[n, h, pl.ds(2 * half, half), cols] = term(of(h, p - 1) + half, half).astype(jnp.bfloat16)
            s0[n, h, pl.ds(3 * half, half), cols] = term(of(h, p + 1), half).astype(jnp.bfloat16)
            send(h, at(s0, h, 0, half), at(r1, h, 0, half), 0, at_first(h, p - 1))
            send(h, at(s0, h, 1, half), at(r1, h, 1, half), 0, at_first(h, p + 1))
            send(h, at(s0, h, 2, half), at(r2, h, 3, half), 1, at_first(h, p - 1))
            send(h, at(s0, h, 3, half), at(r2, h, 2, half), 1, at_first(h, p + 1))

        def stage1():
            p = first[h]
            arrived(h, 0, 2 * half)
            got = r1[n, h, :, cols].astype(jnp.float32)
            s1[n, h, pl.ds(0, half), cols] = (got[:half] + term(of(h, p - 1), half)).astype(jnp.bfloat16)
            s1[n, h, pl.ds(half, half), cols] = (got[half:] + term(of(h, p + 1) + half, half)).astype(jnp.bfloat16)
            send(h, at(s1, h, 0, half), at(r2, h, 0, half), 1, at_first(h, p - 1))
            send(h, at(s1, h, 1, half), at(r2, h, 1, half), 1, at_first(h, p + 1))

        def stage2():
            p, q, t = first[h], second[h], turn(h)
            arrived(h, 1, 4 * half)
            got = r2[n, h, :, cols].astype(jnp.float32)
            rows[n, h, :, cols] = got[:block] + got[block:] + term(of(h, p), block)

            def mine(i):
                return rows[n, h, pl.ds(pl.multiple_of(wrap(i) * sub, sub), sub), cols].astype(jnp.bfloat16)

            s2[n, h, pl.ds(0, sub), cols] = mine(q + 2)
            s2[n, h, pl.ds(sub, sub), cols] = mine(q + t)
            send(h, at(s2, h, 0, sub), at(r3, h, 0, sub), 2, at_second(h, q - t))
            send(h, at(s2, h, 1, sub), at(r4, h, 1, sub), 3, at_second(h, q + t))

        def stage3():
            q, t = second[h], turn(h)
            arrived(h, 2, sub)
            got = r3[n, h, :, cols].astype(jnp.float32)
            s3[n, h, :, cols] = (
                got + rows[n, h, pl.ds(pl.multiple_of(wrap(q - t) * sub, sub), sub), cols]).astype(jnp.bfloat16)
            send(h, at(s3, h, 0, sub), at(r4, h, 0, sub), 3, at_second(h, q - t))

        def stage4():
            p, q = first[h], second[h]
            arrived(h, 3, 2 * sub)
            got = r4[n, h, :, cols].astype(jnp.float32)
            total = got[:sub] + got[sub:] + rows[n, h, pl.ds(pl.multiple_of(q * sub, sub), sub), cols]
            row = of(h, p, q)
            out[n, pl.ds(row, sub), cols] = total.astype(jnp.bfloat16)
            for d in (1, -1):
                send(h, place(row, sub), place(row, sub), 4, at_second(h, q + d))

        def stage5():
            p, q, t = first[h], second[h], turn(h)
            arrived(h, 4, 2 * sub)
            row = of(h, p, q - t)
            send(h, place(row, sub), place(row, sub), 5, at_second(h, q + t))

        def stage6():
            p = first[h]
            arrived(h, 5, sub)
            row = of(h, p)
            for d in (1, -1):
                send(h, place(row, block), place(row, block), 6, at_first(h, p + d))

        def stage7():
            p = first[h]
            arrived(h, 6, 2 * block)
            row = of(h, p - 1)
            send(h, place(row, half), place(row, half), 7, at_first(h, p + 1))
            row = of(h, p + 1) + half
            send(h, place(row, half), place(row, half), 7, at_first(h, p - 1))

        def stage8():
            arrived(h, 7, 2 * half)

        return stage0, stage1, stage2, stage3, stage4, stage5, stage6, stage7, stage8

    def step(it, _):
        for tick in range(2 * per):
            for s in range(len(LAG) - 1, 0, -1):
                back = -((tick - LAG[s]) // (2 * per))
                then = (tick - LAG[s]) % (2 * per)
                n = it - back

                @pl.when((n >= 0) & (n < count))
                def _():
                    stages(n, then // 2, then % 2)[s]()

            @pl.when(it < count)
            def _():
                matmul(it, tick // 2, tick % 2)
                stages(it, tick // 2, tick % 2)[0]()
        return 0

    lax.fori_loop(0, count + -(-LAG[-1] // (2 * per)), step, 0)

    sent = 15 * half_rows // 8
    def finish(n, _):
        for j, (c, w) in enumerate(columns):
            unit = n * per + j
            for h in (0, 1):
                ref = out.at[n, pl.ds(0, sent), pl.ds(c, w)]
                pltpu.make_async_copy(ref, ref, send_sem.at[2 * unit + h]).wait()
        return 0

    lax.fori_loop(0, count, finish, 0)


def solution(mesh):
    def step(a, g):
        a, g = a.reshape(a.shape[1:]), g.reshape(g.shape[1:])
        count, tokens, d_model = a.shape
        ff = g.shape[2]
        assert mesh.shape["dp"] == SIDE * SIDE and sum(TILES) * LANES == ff
        units = count * len(TILES)
        bf16, f32 = jnp.bfloat16, jnp.float32
        half_rows = d_model // 2
        block = half_rows // SIDE
        sub = block // SIDE
        VMEM, DMA = pltpu.VMEM, pltpu.SemaphoreType.DMA
        return pl.pallas_call(
            kernel,
            out_shape=VMEM((count, d_model, ff), bf16),
            in_specs=[pl.BlockSpec(memory_space=pl.ANY)] * 2,
            out_specs=pl.BlockSpec(memory_space=VMEM),
            scratch_shapes=[
                VMEM((2, tokens, d_model), bf16),
                VMEM((2, tokens, max(TILES) * LANES), bf16),
                VMEM((count, d_model, ff), f32),
                VMEM((count, 2, 2 * block, ff), bf16),
                VMEM((count, 2, block, ff), bf16),
                VMEM((count, 2, block, ff), bf16),
                VMEM((count, 2, 2 * block, ff), bf16),
                VMEM((count, 2, block, ff), f32),
                VMEM((count, 2, 2 * sub, ff), bf16),
                VMEM((count, 2, sub, ff), bf16),
                VMEM((count, 2, sub, ff), bf16),
                VMEM((count, 2, 2 * sub, ff), bf16),
                DMA((2, 2)),
                DMA((2,)),
                DMA((2 * units,)),
                DMA((8, 2 * units)),
            ],
            compiler_params=pltpu.CompilerParams(
                collective_id=0, has_side_effects=True, vmem_limit_bytes=57 * 1024 * 1024),
            name="sums",
        )(a, g)

    return jax.shard_map(
        step, mesh=mesh, in_specs=(P(("rep", "dp")), P(("rep", "dp"))), out_specs=P("rep"), check_vma=False)
```

```python
import functools

import jax
import jax.numpy as jnp
from jax import lax
from jax.experimental import pallas as pl
from jax.experimental.pallas import tpu as pltpu
from jax.sharding import PartitionSpec as P

MESH = pl.DeviceIdType.MESH
SIDE = 4
LANES = 128
LAST = 7
TILES = (7, 6)
LAG = (0, 3, 6, 8, 10, 12, 16, 23)
FIRST = 4


def kernel(a_hbm, g_hbm, out, a_buf, g_buf, terms, s0, r1, s1, r2, rows, s2, r3, s3, r4,
           first_sem, a_sem, g_sem, send_sem, recv_sem, last_sem):
    count, tokens, d_model = a_hbm.shape
    columns = []
    for t in TILES:
        columns.append((sum(w for _, w in columns), t * LANES))
    per = len(columns)
    half_rows = d_model // 2
    block = half_rows // SIDE
    side_rows = block // 2
    sub = block // SIDE

    me = lax.axis_index("dp")
    px, py = me // SIDE, me % SIDE
    ring_x = [px] + [(px + i) % SIDE for i in (1, 2, 3)]
    ring_y = [py] + [(py + i) % SIDE for i in (1, 2, 3)]
    first, second = (ring_x, ring_y), (ring_y, ring_x)
    device_x = [p * SIDE + py for p in ring_x]
    device_y = [px * SIDE + p for p in ring_y]
    device_first, device_second = (device_x, device_y), (device_y, device_x)

    def of(h, i, k=None):
        row = h * half_rows + first[h][i % SIDE] * block
        return pl.multiple_of(row if k is None else row + k * sub, sub)

    def a_load(n, h):
        rows_of = pl.ds(h * half_rows, half_rows)
        return pltpu.make_async_copy(a_hbm.at[n, :, rows_of], a_buf.at[n % 2, :, rows_of], a_sem.at[n % 2, h])

    def g_load(n, j):
        c, w = columns[j]
        slot = (n * per + j) % 2
        return pltpu.make_async_copy(g_hbm.at[n, :, pl.ds(c, w)], g_buf.at[slot, :, pl.ds(0, w)], g_sem.at[slot])

    def first_loads(k):
        part = tokens // FIRST
        at, (c, w) = pl.ds(k * part, part), columns[0]
        rows_of = pl.ds(0, half_rows)
        return (pltpu.make_async_copy(a_hbm.at[0, at, rows_of], a_buf.at[0, at, rows_of], first_sem.at[0, k]),
                pltpu.make_async_copy(g_hbm.at[0, at, pl.ds(c, w)], g_buf.at[0, at, pl.ds(0, w)], first_sem.at[1, k]))

    for k in range(FIRST):
        for load in first_loads(k):
            load.start()
    a_load(0, 1).start()
    g_load(0, 1).start()
    a_load(1, 0).start()

    barrier = pltpu.get_barrier_semaphore()
    for i in (1, 3):
        pl.semaphore_signal(barrier, inc=1, device_id={"dp": device_x[i]}, device_id_type=MESH)
        pl.semaphore_signal(barrier, inc=1, device_id={"dp": device_y[i]}, device_id_type=MESH)

    for k in range(FIRST):
        for load in first_loads(k):
            load.wait()
        part, (c, w) = tokens // FIRST, columns[0]
        at = pl.ds(k * part, part)
        term = lax.dot_general(
            a_buf[0, at, pl.ds(0, half_rows)], g_buf[0, at, pl.ds(0, w)],
            (((0,), (0,)), ((), ())), preferred_element_type=jnp.float32)
        if k:
            term += terms[0, pl.ds(0, half_rows), pl.ds(c, w)]
        terms[0, pl.ds(0, half_rows), pl.ds(c, w)] = term

    pl.semaphore_wait(barrier, SIDE)

    def matmul(n, j, h):
        c, w = columns[j]
        if j == 0:
            a_load(n, h).wait()

            @pl.when(n + 1 < count)
            def _():
                a_load(n + 1, h).start()
        if h == 0:
            g_load(n, j).wait()
            if j + 1 < per:
                g_load(n, j + 1).start()
            else:
                @pl.when(n + 1 < count)
                def _():
                    g_load(n + 1, 0).start()
        mine = pl.ds(h * half_rows, half_rows)
        terms[n, mine, pl.ds(c, w)] = lax.dot_general(
            a_buf[n % 2, :, mine], g_buf[(n * per + j) % 2, :, pl.ds(0, w)],
            (((0,), (0,)), ((), ())), preferred_element_type=jnp.float32)

    def stages(n, j, h):
        c, w = columns[j]
        cols = pl.ds(c, w)
        unit = n * per + j

        def term(row, size):
            return terms[n, pl.ds(row, size), cols]

        def send(src, dst, kind, device):
            pltpu.make_async_remote_copy(
                src_ref=src, dst_ref=dst, send_sem=send_sem.at[n],
                recv_sem=last_sem.at[n] if kind == LAST else recv_sem.at[kind, 2 * unit + h],
                device_id={"dp": device}, device_id_type=MESH).start()

        def arrived(kind, size):
            ref = out.at[n, pl.ds(0, size), cols]
            pltpu.make_async_copy(ref, ref, recv_sem.at[kind, 2 * unit + h]).wait()

        p, q = first[h], second[h]
        up, down = device_first[h][1], device_first[h][3]
        odd = (unit + h) % 2
        ahead, behind = q[1] + odd * (q[3] - q[1]), q[3] + odd * (q[1] - q[3])
        to = device_second[h]
        to_ahead, to_behind = to[1] + odd * (to[3] - to[1]), to[3] + odd * (to[1] - to[3])

        def at(buf, i, size):
            return buf.at[n, h, pl.ds(i * size, size), cols]

        def place(row, size):
            return out.at[n, pl.ds(row, size), cols]

        def mine(i):
            return rows[n, h, pl.ds(pl.multiple_of(i * sub, sub), sub), cols]

        half = side_rows

        def stage0():
            s0[n, h, pl.ds(0, block), cols] = term(of(h, 2), block).astype(jnp.bfloat16)
            s0[n, h, pl.ds(2 * half, half), cols] = term(of(h, 3) + half, half).astype(jnp.bfloat16)
            s0[n, h, pl.ds(3 * half, half), cols] = term(of(h, 1), half).astype(jnp.bfloat16)
            send(at(s0, 0, half), at(r1, 0, half), 0, down)
            send(at(s0, 1, half), at(r1, 1, half), 0, up)
            send(at(s0, 2, half), at(r2, 3, half), 1, down)
            send(at(s0, 3, half), at(r2, 2, half), 1, up)

        def stage1():
            arrived(0, 2 * half)
            got = r1[n, h, :, cols].astype(jnp.float32)
            s1[n, h, pl.ds(0, half), cols] = (got[:half] + term(of(h, 3), half)).astype(jnp.bfloat16)
            s1[n, h, pl.ds(half, half), cols] = (got[half:] + term(of(h, 1) + half, half)).astype(jnp.bfloat16)
            send(at(s1, 0, half), at(r2, 0, half), 1, down)
            send(at(s1, 1, half), at(r2, 1, half), 1, up)

        def stage2():
            arrived(1, 4 * half)
            got = r2[n, h, :, cols].astype(jnp.float32)
            rows[n, h, :, cols] = got[:block] + got[block:] + term(of(h, 0), block)
            s2[n, h, pl.ds(0, sub), cols] = mine(q[2]).astype(jnp.bfloat16)
            s2[n, h, pl.ds(sub, sub), cols] = mine(ahead).astype(jnp.bfloat16)
            send(at(s2, 0, sub), at(r3, 0, sub), 2, to_behind)
            send(at(s2, 1, sub), at(r4, 1, sub), 3, to_ahead)

        def stage3():
            arrived(2, sub)
            s3[n, h, :, cols] = (r3[n, h, :, cols].astype(jnp.float32) + mine(behind)).astype(jnp.bfloat16)
            send(at(s3, 0, sub), at(r4, 0, sub), 3, to_behind)

        def stage4():
            arrived(3, 2 * sub)
            got = r4[n, h, :, cols].astype(jnp.float32)
            row = of(h, 0, q[0])
            out[n, pl.ds(row, sub), cols] = (got[:sub] + got[sub:] + mine(q[0])).astype(jnp.bfloat16)
            for i in (1, 3):
                send(place(row, sub), place(row, sub), 4, to[i])

        def stage5():
            arrived(4, 2 * sub)
            row = of(h, 0, behind)
            send(place(row, sub), place(row, sub), 5, to_ahead)

        def stage6():
            arrived(5, sub)
            row = of(h, 0)
            send(place(row, block), place(row, block), 6, up)
            send(place(row, block), place(row, block), 6, down)

        def stage7():
            arrived(6, 2 * block)
            row = of(h, 3)
            send(place(row, half), place(row, half), LAST, up)
            row = of(h, 1) + half
            send(place(row, half), place(row, half), LAST, down)

        return stage0, stage1, stage2, stage3, stage4, stage5, stage6, stage7

    def step(it, _):
        for tick in range(2 * per):
            @pl.when(it < count)
            def _():
                stages(it, tick // 2, tick % 2)[0]()

            for s in range(len(LAG) - 1, 0, -1):
                back = -((tick - LAG[s]) // (2 * per))
                then = (tick - LAG[s]) % (2 * per)
                n = it - back

                @pl.when((n >= 0) & (n < count))
                def _():
                    stages(n, then // 2, then % 2)[s]()

            later = (tick + 1) % (2 * per)
            n = it if later else it + 1

            @pl.when(n < count)
            def _():
                matmul(n, later // 2, later % 2)
        return 0

    lax.fori_loop(0, count + -(-LAG[-1] // (2 * per)), step, 0)

    def finish(n, _):
        ref = out.at[pl.ds(0, 2), pl.ds(0, 15 * half_rows // 8)]
        pltpu.make_async_copy(ref, ref, send_sem.at[n]).wait()
        ref = out.at[0, pl.ds(0, 4 * side_rows)]
        pltpu.make_async_copy(ref, ref, last_sem.at[n]).wait()
        return 0

    lax.fori_loop(0, count, finish, 0)


def solution(mesh):
    def step(a, g):
        a, g = a.reshape(a.shape[1:]), g.reshape(g.shape[1:])
        count, tokens, d_model = a.shape
        ff = g.shape[2]
        assert mesh.shape["dp"] == SIDE * SIDE and sum(TILES) * LANES == ff
        units = count * len(TILES)
        bf16, f32 = jnp.bfloat16, jnp.float32
        half_rows = d_model // 2
        block = half_rows // SIDE
        sub = block // SIDE
        VMEM, DMA = pltpu.VMEM, pltpu.SemaphoreType.DMA
        return pl.pallas_call(
            kernel,
            out_shape=VMEM((count, d_model, ff), bf16),
            in_specs=[pl.BlockSpec(memory_space=pl.ANY)] * 2,
            out_specs=pl.BlockSpec(memory_space=VMEM),
            scratch_shapes=[
                VMEM((2, tokens, d_model), bf16),
                VMEM((2, tokens, max(TILES) * LANES), bf16),
                VMEM((count, d_model, ff), f32),
                VMEM((count, 2, 2 * block, ff), bf16),
                VMEM((count, 2, block, ff), bf16),
                VMEM((count, 2, block, ff), bf16),
                VMEM((count, 2, 2 * block, ff), bf16),
                VMEM((count, 2, block, ff), f32),
                VMEM((count, 2, 2 * sub, ff), bf16),
                VMEM((count, 2, sub, ff), bf16),
                VMEM((count, 2, sub, ff), bf16),
                VMEM((count, 2, 2 * sub, ff), bf16),
                DMA((2, FIRST)),
                DMA((2, 2)),
                DMA((2,)),
                DMA((count,)),
                DMA((LAST, 2 * units)),
                DMA((count,)),
            ],
            compiler_params=pltpu.CompilerParams(
                collective_id=0, has_side_effects=True, vmem_limit_bytes=57 * 1024 * 1024),
            name="sums",
        )(a, g)

    return jax.shard_map(
        step, mesh=mesh, in_specs=(P(("rep", "dp")), P(("rep", "dp"))), out_specs=P("rep"), check_vma=False)
```

```python
import functools

import jax
import jax.numpy as jnp
from jax import lax
from jax.experimental import pallas as pl
from jax.experimental.pallas import tpu as pltpu
from jax.sharding import PartitionSpec as P

MESH = pl.DeviceIdType.MESH
SIDE = 4
LANES = 128
LAST = 7
SHARED = (0, 1, 2, 3, 1, 2, 0)
TILES = (7, 6)
LAG = (0, 3, 6, 8, 10, 12, 16, 23)
ORDER = (7, 6, 5, 4, 3, 2, 1)
FIRST = 4


def kernel(a_hbm, g_hbm, out, a_buf, g_buf, terms, s0, r1, s1, r2, rows, s2, r3, s3, r4,
           first_sem, a_sem, g_sem, send_sem, recv_sem, last_sem):
    count, tokens, d_model = a_hbm.shape
    columns = []
    for t in TILES:
        columns.append((sum(w for _, w in columns), t * LANES))
    per = len(columns)
    half_rows = d_model // 2
    block = half_rows // SIDE
    side_rows = block // 2
    sub = block // SIDE

    me = lax.axis_index("dp")
    px, py = me // SIDE, me % SIDE
    ring_x = [px] + [(px + i) % SIDE for i in (1, 2, 3)]
    ring_y = [py] + [(py + i) % SIDE for i in (1, 2, 3)]
    first, second = (ring_x, ring_y), (ring_y, ring_x)
    device_x = [p * SIDE + py for p in ring_x]
    device_y = [px * SIDE + p for p in ring_y]
    device_first, device_second = (device_x, device_y), (device_y, device_x)

    def of(h, i, k=None):
        row = h * half_rows + first[h][i % SIDE] * block
        return pl.multiple_of(row if k is None else row + k * sub, sub)

    def a_load(n, h):
        rows_of = pl.ds(h * half_rows, half_rows)
        return pltpu.make_async_copy(a_hbm.at[n, :, rows_of], a_buf.at[n % 2, :, rows_of], a_sem.at[n % 2, h])

    def g_load(n, j):
        c, w = columns[j]
        slot = (n * per + j) % 2
        return pltpu.make_async_copy(g_hbm.at[n, :, pl.ds(c, w)], g_buf.at[slot, :, pl.ds(0, w)], g_sem.at[slot])

    def first_loads(k):
        part = tokens // FIRST
        at, (c, w) = pl.ds(k * part, part), columns[0]
        rows_of = pl.ds(0, half_rows)
        return (pltpu.make_async_copy(a_hbm.at[0, at, rows_of], a_buf.at[0, at, rows_of], first_sem.at[0, k]),
                pltpu.make_async_copy(g_hbm.at[0, at, pl.ds(c, w)], g_buf.at[0, at, pl.ds(0, w)], first_sem.at[1, k]))

    for k in range(FIRST):
        for load in first_loads(k):
            load.start()
    a_load(0, 1).start()
    g_load(0, 1).start()
    a_load(1, 0).start()

    barrier = pltpu.get_barrier_semaphore()
    for i in (1, 3):
        pl.semaphore_signal(barrier, inc=1, device_id={"dp": device_x[i]}, device_id_type=MESH)
        pl.semaphore_signal(barrier, inc=1, device_id={"dp": device_y[i]}, device_id_type=MESH)

    for k in range(FIRST):
        for load in first_loads(k):
            load.wait()
        part, (c, w) = tokens // FIRST, columns[0]
        at = pl.ds(k * part, part)
        term = lax.dot_general(
            a_buf[0, at, pl.ds(0, half_rows)], g_buf[0, at, pl.ds(0, w)],
            (((0,), (0,)), ((), ())), preferred_element_type=jnp.float32)
        if k:
            term += terms[0, pl.ds(0, half_rows), pl.ds(c, w)]
        terms[0, pl.ds(0, half_rows), pl.ds(c, w)] = term

    pl.semaphore_wait(barrier, SIDE)

    def matmul(n, j, h):
        c, w = columns[j]
        if j == 0:
            a_load(n, h).wait()

            @pl.when(n + 1 < count)
            def _():
                a_load(n + 1, h).start()
        if h == 0:
            g_load(n, j).wait()
            if j + 1 < per:
                g_load(n, j + 1).start()
            else:
                @pl.when(n + 1 < count)
                def _():
                    g_load(n + 1, 0).start()
        mine = pl.ds(h * half_rows, half_rows)
        terms[n, mine, pl.ds(c, w)] = lax.dot_general(
            a_buf[n % 2, :, mine], g_buf[(n * per + j) % 2, :, pl.ds(0, w)],
            (((0,), (0,)), ((), ())), preferred_element_type=jnp.float32)

    def stages(n, j, h):
        c, w = columns[j]
        cols = pl.ds(c, w)
        unit = n * per + j

        def term(row, size):
            return terms[n, pl.ds(row, size), cols]

        def send(src, dst, kind, device):
            pltpu.make_async_remote_copy(
                src_ref=src, dst_ref=dst, send_sem=send_sem.at[n],
                recv_sem=last_sem.at[n] if kind == LAST else recv_sem.at[SHARED[kind], 2 * unit + h],
                device_id={"dp": device}, device_id_type=MESH).start()

        def arrived(kind, size):
            ref = out.at[n, pl.ds(0, size), cols]
            pltpu.make_async_copy(ref, ref, recv_sem.at[SHARED[kind], 2 * unit + h]).wait()

        p, q = first[h], second[h]
        up, down = device_first[h][1], device_first[h][3]
        odd = (unit + h) % 2
        ahead, behind = q[1] + odd * (q[3] - q[1]), q[3] + odd * (q[1] - q[3])
        to = device_second[h]
        to_ahead, to_behind = to[1] + odd * (to[3] - to[1]), to[3] + odd * (to[1] - to[3])

        def at(buf, i, size):
            return buf.at[n, h, pl.ds(i * size, size), cols]

        def place(row, size):
            return out.at[n, pl.ds(row, size), cols]

        def mine(i):
            return rows[n, h, pl.ds(pl.multiple_of(i * sub, sub), sub), cols]

        half = side_rows

        def stage0():
            s0[n, h, pl.ds(0, block), cols] = term(of(h, 2), block).astype(jnp.bfloat16)
            s0[n, h, pl.ds(2 * half, half), cols] = term(of(h, 3) + half, half).astype(jnp.bfloat16)
            s0[n, h, pl.ds(3 * half, half), cols] = term(of(h, 1), half).astype(jnp.bfloat16)
            send(at(s0, 0, half), at(r1, 0, half), 0, down)
            send(at(s0, 1, half), at(r1, 1, half), 0, up)
            send(at(s0, 2, half), at(r2, 3, half), 1, down)
            send(at(s0, 3, half), at(r2, 2, half), 1, up)

        def stage1():
            arrived(0, 2 * half)
            got = r1[n, h, :, cols].astype(jnp.float32)
            s1[n, h, pl.ds(0, half), cols] = (got[:half] + term(of(h, 3), half)).astype(jnp.bfloat16)
            s1[n, h, pl.ds(half, half), cols] = (got[half:] + term(of(h, 1) + half, half)).astype(jnp.bfloat16)
            send(at(s1, 0, half), at(r2, 0, half), 1, down)
            send(at(s1, 1, half), at(r2, 1, half), 1, up)

        def stage2():
            arrived(1, 4 * half)
            got = r2[n, h, :, cols].astype(jnp.float32)
            rows[n, h, :, cols] = got[:block] + got[block:] + term(of(h, 0), block)
            s2[n, h, pl.ds(0, sub), cols] = mine(q[2]).astype(jnp.bfloat16)
            s2[n, h, pl.ds(sub, sub), cols] = mine(ahead).astype(jnp.bfloat16)
            send(at(s2, 0, sub), at(r3, 0, sub), 2, to_behind)
            send(at(s2, 1, sub), at(r4, 1, sub), 3, to_ahead)

        def stage3():
            arrived(2, sub)
            s3[n, h, :, cols] = (r3[n, h, :, cols].astype(jnp.float32) + mine(behind)).astype(jnp.bfloat16)
            send(at(s3, 0, sub), at(r4, 0, sub), 3, to_behind)

        def stage4():
            arrived(3, 2 * sub)
            got = r4[n, h, :, cols].astype(jnp.float32)
            row = of(h, 0, q[0])
            out[n, pl.ds(row, sub), cols] = (got[:sub] + got[sub:] + mine(q[0])).astype(jnp.bfloat16)
            for i in (1, 3):
                send(place(row, sub), place(row, sub), 4, to[i])

        def stage5():
            arrived(4, 2 * sub)
            row = of(h, 0, behind)
            send(place(row, sub), place(row, sub), 5, to_ahead)

        def stage6():
            arrived(5, sub)
            row = of(h, 0)
            send(place(row, block), place(row, block), 6, up)
            send(place(row, block), place(row, block), 6, down)

        def stage7():
            arrived(6, 2 * block)
            row = of(h, 3)
            send(place(row, half), place(row, half), LAST, up)
            row = of(h, 1) + half
            send(place(row, half), place(row, half), LAST, down)

        return stage0, stage1, stage2, stage3, stage4, stage5, stage6, stage7

    def step(it, _):
        for tick in range(2 * per):
            @pl.when(it < count)
            def _():
                stages(it, tick // 2, tick % 2)[0]()

            for s in ORDER:
                back = -((tick - LAG[s]) // (2 * per))
                then = (tick - LAG[s]) % (2 * per)
                n = it - back

                @pl.when((n >= 0) & (n < count))
                def _():
                    stages(n, then // 2, then % 2)[s]()

            later = (tick + 1) % (2 * per)
            n = it if later else it + 1

            @pl.when(n < count)
            def _():
                matmul(n, later // 2, later % 2)
        return 0

    lax.fori_loop(0, count + -(-LAG[-1] // (2 * per)), step, 0)

    def finish(n, _):
        ref = out.at[pl.ds(0, 2), pl.ds(0, 15 * half_rows // 8)]
        pltpu.make_async_copy(ref, ref, send_sem.at[n]).wait()
        ref = out.at[0, pl.ds(0, 4 * side_rows)]
        pltpu.make_async_copy(ref, ref, last_sem.at[n]).wait()
        return 0

    lax.fori_loop(0, count, finish, 0)


def solution(mesh):
    def step(a, g):
        a, g = a.reshape(a.shape[1:]), g.reshape(g.shape[1:])
        count, tokens, d_model = a.shape
        ff = g.shape[2]
        assert mesh.shape["dp"] == SIDE * SIDE and sum(TILES) * LANES == ff
        units = count * len(TILES)
        bf16, f32 = jnp.bfloat16, jnp.float32
        half_rows = d_model // 2
        block = half_rows // SIDE
        sub = block // SIDE
        VMEM, DMA = pltpu.VMEM, pltpu.SemaphoreType.DMA
        return pl.pallas_call(
            kernel,
            out_shape=VMEM((count, d_model, ff), bf16),
            in_specs=[pl.BlockSpec(memory_space=pl.ANY)] * 2,
            out_specs=pl.BlockSpec(memory_space=VMEM),
            scratch_shapes=[
                VMEM((2, tokens, d_model), bf16),
                VMEM((2, tokens, max(TILES) * LANES), bf16),
                VMEM((count, d_model, ff), f32),
                VMEM((count, 2, 2 * block, ff), bf16),
                VMEM((count, 2, block, ff), bf16),
                VMEM((count, 2, block, ff), bf16),
                VMEM((count, 2, 2 * block, ff), bf16),
                VMEM((count, 2, block, ff), f32),
                VMEM((count, 2, 2 * sub, ff), bf16),
                VMEM((count, 2, sub, ff), bf16),
                VMEM((count, 2, sub, ff), bf16),
                VMEM((count, 2, 2 * sub, ff), bf16),
                DMA((2, FIRST)),
                DMA((2, 2)),
                DMA((2,)),
                DMA((count,)),
                DMA((max(SHARED) + 1, 2 * units)),
                DMA((count,)),
            ],
            compiler_params=pltpu.CompilerParams(
                collective_id=0, has_side_effects=True, vmem_limit_bytes=57 * 1024 * 1024),
            name="sums",
        )(a, g)

    return jax.shard_map(
        step, mesh=mesh, in_specs=(P(("rep", "dp")), P(("rep", "dp"))), out_specs=P("rep"), check_vma=False)
```

```python
import functools

import jax
import jax.numpy as jnp
from jax import lax
from jax.experimental import pallas as pl
from jax.experimental.pallas import tpu as pltpu
from jax.sharding import PartitionSpec as P

MESH = pl.DeviceIdType.MESH
SIDE = 4
LANES = 128
LAST = 7
SHARED = (0, 1, 2, 3, 1, 2, 0)
TILES = (7, 6)
LAG = (0, 3, 6, 8, 10, 12, 16, 25)
ORDER = (7, 6, 5, 4, 3, 2, 1)
FIRST = 4


def kernel(a_hbm, g_hbm, out, a_buf, g_buf, terms, s0, r1, s1, r2, rows, s2, r3, s3, r4,
           first_sem, a_sem, g_sem, send_sem, recv_sem, last_sem):
    count, tokens, d_model = a_hbm.shape
    columns = []
    for t in TILES:
        columns.append((sum(w for _, w in columns), t * LANES))
    per = len(columns)
    half_rows = d_model // 2
    block = half_rows // SIDE
    side_rows = block // 2
    sub = block // SIDE

    me = lax.axis_index("dp")
    px, py = me // SIDE, me % SIDE
    ring_x = [px] + [(px + i) % SIDE for i in (1, 2, 3)]
    ring_y = [py] + [(py + i) % SIDE for i in (1, 2, 3)]
    first, second = (ring_x, ring_y), (ring_y, ring_x)
    device_x = [p * SIDE + py for p in ring_x]
    device_y = [px * SIDE + p for p in ring_y]
    device_first, device_second = (device_x, device_y), (device_y, device_x)

    def of(h, i, k=None):
        row = h * half_rows + first[h][i % SIDE] * block
        return pl.multiple_of(row if k is None else row + k * sub, sub)

    def a_load(n, h):
        rows_of = pl.ds(h * half_rows, half_rows)
        return pltpu.make_async_copy(a_hbm.at[n, :, rows_of], a_buf.at[n % 2, :, rows_of], a_sem.at[n % 2, h])

    def g_load(n, j):
        c, w = columns[j]
        slot = (n * per + j) % 2
        return pltpu.make_async_copy(g_hbm.at[n, :, pl.ds(c, w)], g_buf.at[slot, :, pl.ds(0, w)], g_sem.at[slot])

    def first_loads(k):
        part = tokens // FIRST
        at, (c, w) = pl.ds(k * part, part), columns[0]
        rows_of = pl.ds(0, half_rows)
        return (pltpu.make_async_copy(a_hbm.at[0, at, rows_of], a_buf.at[0, at, rows_of], first_sem.at[0, k]),
                pltpu.make_async_copy(g_hbm.at[0, at, pl.ds(c, w)], g_buf.at[0, at, pl.ds(0, w)], first_sem.at[1, k]))

    for k in range(FIRST):
        for load in first_loads(k):
            load.start()
    a_load(0, 1).start()
    g_load(0, 1).start()
    a_load(1, 0).start()

    barrier = pltpu.get_barrier_semaphore()
    for i in (1, 3):
        pl.semaphore_signal(barrier, inc=1, device_id={"dp": device_x[i]}, device_id_type=MESH)
        pl.semaphore_signal(barrier, inc=1, device_id={"dp": device_y[i]}, device_id_type=MESH)

    for k in range(FIRST):
        for load in first_loads(k):
            load.wait()
        part, (c, w) = tokens // FIRST, columns[0]
        at = pl.ds(k * part, part)
        term = lax.dot_general(
            a_buf[0, at, pl.ds(0, half_rows)], g_buf[0, at, pl.ds(0, w)],
            (((0,), (0,)), ((), ())), preferred_element_type=jnp.float32)
        if k:
            term += terms[0, pl.ds(0, half_rows), pl.ds(c, w)]
        terms[0, pl.ds(0, half_rows), pl.ds(c, w)] = term

    pl.semaphore_wait(barrier, SIDE)

    def matmul(n, j, h):
        c, w = columns[j]
        if j == 0:
            a_load(n, h).wait()

            @pl.when(n + 1 < count)
            def _():
                a_load(n + 1, h).start()
        if h == 0:
            g_load(n, j).wait()
            if j + 1 < per:
                g_load(n, j + 1).start()
            else:
                @pl.when(n + 1 < count)
                def _():
                    g_load(n + 1, 0).start()
        mine = pl.ds(h * half_rows, half_rows)
        terms[n, mine, pl.ds(c, w)] = lax.dot_general(
            a_buf[n % 2, :, mine], g_buf[(n * per + j) % 2, :, pl.ds(0, w)],
            (((0,), (0,)), ((), ())), preferred_element_type=jnp.float32)

    def stages(n, j, h):
        c, w = columns[j]
        cols = pl.ds(c, w)
        unit = n * per + j

        def term(row, size):
            return terms[n, pl.ds(row, size), cols]

        def send(src, dst, kind, device):
            pltpu.make_async_remote_copy(
                src_ref=src, dst_ref=dst, send_sem=send_sem.at[n],
                recv_sem=last_sem.at[n] if kind == LAST else recv_sem.at[SHARED[kind], 2 * unit + h],
                device_id={"dp": device}, device_id_type=MESH).start()

        def arrived(kind, size):
            ref = out.at[n, pl.ds(0, size), cols]
            pltpu.make_async_copy(ref, ref, recv_sem.at[SHARED[kind], 2 * unit + h]).wait()

        p, q = first[h], second[h]
        up, down = device_first[h][1], device_first[h][3]
        odd = (unit + h) % 2
        ahead, behind = q[1] + odd * (q[3] - q[1]), q[3] + odd * (q[1] - q[3])
        to = device_second[h]
        to_ahead, to_behind = to[1] + odd * (to[3] - to[1]), to[3] + odd * (to[1] - to[3])

        def at(buf, i, size):
            return buf.at[n, h, pl.ds(i * size, size), cols]

        def place(row, size):
            return out.at[n, pl.ds(row, size), cols]

        def mine(i):
            return rows[n, h, pl.ds(pl.multiple_of(i * sub, sub), sub), cols]

        half = side_rows

        def stage0():
            s0[n, h, pl.ds(0, block), cols] = term(of(h, 2), block).astype(jnp.bfloat16)
            s0[n, h, pl.ds(2 * half, half), cols] = term(of(h, 3) + half, half).astype(jnp.bfloat16)
            s0[n, h, pl.ds(3 * half, half), cols] = term(of(h, 1), half).astype(jnp.bfloat16)
            send(at(s0, 0, half), at(r1, 0, half), 0, down)
            send(at(s0, 1, half), at(r1, 1, half), 0, up)
            send(at(s0, 2, half), at(r2, 3, half), 1, down)
            send(at(s0, 3, half), at(r2, 2, half), 1, up)

        def stage1():
            arrived(0, 2 * half)
            got = r1[n, h, :, cols].astype(jnp.float32)
            s1[n, h, pl.ds(0, half), cols] = (got[:half] + term(of(h, 3), half)).astype(jnp.bfloat16)
            s1[n, h, pl.ds(half, half), cols] = (got[half:] + term(of(h, 1) + half, half)).astype(jnp.bfloat16)
            send(at(s1, 0, half), at(r2, 0, half), 1, down)
            send(at(s1, 1, half), at(r2, 1, half), 1, up)

        def stage2():
            arrived(1, 4 * half)
            got = r2[n, h, :, cols].astype(jnp.float32)
            rows[n, h, :, cols] = got[:block] + got[block:] + term(of(h, 0), block)
            s2[n, h, pl.ds(0, sub), cols] = mine(q[2]).astype(jnp.bfloat16)
            s2[n, h, pl.ds(sub, sub), cols] = mine(ahead).astype(jnp.bfloat16)
            send(at(s2, 0, sub), at(r3, 0, sub), 2, to_behind)
            send(at(s2, 1, sub), at(r4, 1, sub), 3, to_ahead)

        def stage3():
            arrived(2, sub)
            s3[n, h, :, cols] = (r3[n, h, :, cols].astype(jnp.float32) + mine(behind)).astype(jnp.bfloat16)
            send(at(s3, 0, sub), at(r4, 0, sub), 3, to_behind)

        def stage4():
            arrived(3, 2 * sub)
            got = r4[n, h, :, cols].astype(jnp.float32)
            row = of(h, 0, q[0])
            out[n, pl.ds(row, sub), cols] = (got[:sub] + got[sub:] + mine(q[0])).astype(jnp.bfloat16)
            for i in (1, 3):
                send(place(row, sub), place(row, sub), 4, to[i])

        def stage5():
            arrived(4, 2 * sub)
            row = of(h, 0, behind)
            send(place(row, sub), place(row, sub), 5, to_ahead)

        def stage6():
            arrived(5, sub)
            row = of(h, 0)
            send(place(row, block), place(row, block), 6, up)
            send(place(row, block), place(row, block), 6, down)

        def stage7():
            arrived(6, 2 * block)
            row = of(h, 3)
            send(place(row, half), place(row, half), LAST, up)
            row = of(h, 1) + half
            send(place(row, half), place(row, half), LAST, down)

        return stage0, stage1, stage2, stage3, stage4, stage5, stage6, stage7

    def step(it, _):
        for tick in range(2 * per):
            @pl.when(it < count)
            def _():
                stages(it, tick // 2, tick % 2)[0]()

            for s in ORDER:
                back = -((tick - LAG[s]) // (2 * per))
                then = (tick - LAG[s]) % (2 * per)
                n = it - back

                @pl.when((n >= 0) & (n < count))
                def _():
                    stages(n, then // 2, then % 2)[s]()

            later = (tick + 1) % (2 * per)
            n = it if later else it + 1

            @pl.when(n < count)
            def _():
                matmul(n, later // 2, later % 2)
        return 0

    lax.fori_loop(0, count + -(-LAG[-1] // (2 * per)), step, 0)

    def finish(n, _):
        ref = out.at[pl.ds(0, 2), pl.ds(0, 15 * half_rows // 8)]
        pltpu.make_async_copy(ref, ref, send_sem.at[n]).wait()
        ref = out.at[0, pl.ds(0, 4 * side_rows)]
        pltpu.make_async_copy(ref, ref, last_sem.at[n]).wait()
        return 0

    lax.fori_loop(0, count, finish, 0)


def solution(mesh):
    def step(a, g):
        a, g = a.reshape(a.shape[1:]), g.reshape(g.shape[1:])
        count, tokens, d_model = a.shape
        ff = g.shape[2]
        assert mesh.shape["dp"] == SIDE * SIDE and sum(TILES) * LANES == ff
        units = count * len(TILES)
        bf16, f32 = jnp.bfloat16, jnp.float32
        half_rows = d_model // 2
        block = half_rows // SIDE
        sub = block // SIDE
        VMEM, DMA = pltpu.VMEM, pltpu.SemaphoreType.DMA
        return pl.pallas_call(
            kernel,
            out_shape=VMEM((count, d_model, ff), bf16),
            in_specs=[pl.BlockSpec(memory_space=pl.ANY)] * 2,
            out_specs=pl.BlockSpec(memory_space=VMEM),
            scratch_shapes=[
                VMEM((2, tokens, d_model), bf16),
                VMEM((2, tokens, max(TILES) * LANES), bf16),
                VMEM((count, d_model, ff), f32),
                VMEM((count, 2, 2 * block, ff), bf16),
                VMEM((count, 2, block, ff), bf16),
                VMEM((count, 2, block, ff), bf16),
                VMEM((count, 2, 2 * block, ff), bf16),
                VMEM((count, 2, block, ff), f32),
                VMEM((count, 2, 2 * sub, ff), bf16),
                VMEM((count, 2, sub, ff), bf16),
                VMEM((count, 2, sub, ff), bf16),
                VMEM((count, 2, 2 * sub, ff), bf16),
                DMA((2, FIRST)),
                DMA((2, 2)),
                DMA((2,)),
                DMA((count,)),
                DMA((max(SHARED) + 1, 2 * units)),
                DMA((count,)),
            ],
            compiler_params=pltpu.CompilerParams(
                collective_id=0, has_side_effects=True, vmem_limit_bytes=57 * 1024 * 1024),
            name="sums",
        )(a, g)

    return jax.shard_map(
        step, mesh=mesh, in_specs=(P(("rep", "dp")), P(("rep", "dp"))), out_specs=P("rep"), check_vma=False)
```
